32 devices in a mesh: grp: 2 (over x), seq: 16 (over z, y, core).
Axes of the slice: x: 2, y: 2, z: 4, core: 2. Of those that a mesh axis runs over, the one named last changes fastest.
Arguments:
- llm_grad: bfloat16 [4096, 8192], P('seq', 'grp'), may hold values from -6 to 6
- image_grid: int32 [256, 2], replicated, may hold values from 1 to 3, as said below
- image_owner: int32 [256], replicated, may hold values from 0 to 15, as said below
- row_start: int32 [256], replicated, may hold values from 0 to 255, as said below
- merger_pre: bfloat16 [48, 16, 2560], P(None, 'seq', 'grp'), may hold values from -6 to 6
- vit_out: bfloat16 [192, 16, 1280], P(None, 'seq'), may hold values from -6 to 6
- vit_pre: bfloat16 [192, 16, 2560], P(None, 'seq', 'grp'), may hold values from -6 to 6
- ln_gain: float32 [1280], replicated, may hold values from 0.25 to 1.75
- merger_out_w: bfloat16 [8192, 2560], P('seq', 'grp'), may hold values from -0.0625 to 0.0625
- merger_in_w: bfloat16 [2560, 5120], P('grp', 'seq'), may hold values from -0.125 to 0.125
- vit_fc2_w: bfloat16 [1280, 2560], P('seq', 'grp'), may hold values from -0.15625 to 0.15625
Outputs:
- patch_grad: bfloat16 [192, 16, 1280], P('grp', 'seq')
- fc1_grad: bfloat16 [192, 16, 2560], P(None, 'seq', 'grp')
- fc2_w_grad: float32 [1280, 2560], P('seq', 'grp')
The draws below stay inside these ranges and needn't reach their ends.
Inputs may be any that keep to these rules, and one draw needn't show every extreme that they name: `image_grid`: height times width is 1 to 3; the first image of every shard is 1 by 3; the last image of shard 0 is 1 by 1. `image_owner`: the 16 images of one shard have 16 different owners. An image's rows row_start to row_start + t - 1 lie inside its shard and meet no other image's rows; a shard's images follow the order of k; the last image of every shard ends at the shard's last row; the first image of shard 0 starts at row 0.
All inputs are finite; a program needn't handle non-finite values.
Results may differ from the reference program's by a relative error of at most 0.02.
Values may be sent and summed in bfloat16 or wider, within the bound.
A program may use at most 128 MiB of HBM per device.

```python
import jax
import jax.numpy as jnp
from jax import lax

D_LLM = 8192
VIT = 1280
HID = 2560
VHID = 2560
SLOT = 3
SEQ_TOK = 256
MERGE_IN = 5120
IMAGES = 256
MROWS = 48
PSLOT = 192
LLM_TOK = 4096
N_GRP = 2
N_SEQ = 16


def image_layout(key):
    shape_ids = jax.random.randint(jax.random.fold_in(key, 101), (N_SEQ, N_SEQ), 0, 5)
    shape_ids = shape_ids.at[:, 0].set(3)
    shape_ids = shape_ids.at[0, N_SEQ - 1].set(0)
    heights = jnp.array([1, 1, 2, 1, 3], jnp.int32)[shape_ids]
    widths = jnp.array([1, 2, 1, 3, 1], jnp.int32)[shape_ids]
    owner_keys = jax.random.split(jax.random.fold_in(key, 202), N_SEQ)
    owners = jax.vmap(lambda one_key: jax.random.permutation(one_key, N_SEQ))(owner_keys).astype(jnp.int32)
    most_gap = (SEQ_TOK - SLOT * N_SEQ) // N_SEQ
    gap_rows = jax.random.randint(jax.random.fold_in(key, 303), (N_SEQ, N_SEQ), 0, most_gap + 1)
    gap_rows = gap_rows.at[0, 0].set(0)
    token_counts = heights * widths
    span_rows = gap_rows + token_counts
    starts = jnp.cumsum(span_rows, axis=1) - token_counts
    starts = starts.at[:, N_SEQ - 1].set(SEQ_TOK - token_counts[:, N_SEQ - 1])
    return (heights, widths, owners, starts.astype(jnp.int32))


def draw_image_grid(key, part):
    heights, widths, owners, starts = image_layout(key)
    return jnp.stack([heights, widths], -1).reshape(IMAGES, 2).astype(jnp.int32)


def draw_image_owner(key, part):
    heights, widths, owners, starts = image_layout(key)
    return owners.reshape(IMAGES)


def draw_row_start(key, part):
    heights, widths, owners, starts = image_layout(key)
    return starts.reshape(IMAGES)


def shard_levels(key, extent, cuts, least, largest):
    gain = 1.0
    for dim, shards_of in cuts:
        steps = jax.random.uniform(jax.random.fold_in(jax.random.fold_in(key, 6), dim), (shards_of,), jnp.float32, least / len(cuts), largest / len(cuts))
        gain = gain * jnp.repeat(jnp.exp(steps), extent[dim] // shards_of).reshape((-1,) + (1,) * (len(extent) - 1 - dim))
    return gain


def gaussian(own_key, shape, spread, reach, cuts=(), kind=jnp.bfloat16):
    entries = jax.random.normal(own_key, shape, jnp.float32) * spread
    if len(cuts) > 0:
        entries = shard_levels(own_key, shape, cuts, -0.22, 0.18) * entries
    return jnp.clip(entries, min=-reach, max=reach).astype(kind)


def setup_inputs(seed: int = 0) -> dict:
    seeds = jax.random.split(jax.random.key(seed), 12)
    return {
        "llm_grad": gaussian(seeds[0], (LLM_TOK, D_LLM), 1.0, 6.0, ((0, 16), (1, 2))),
        "image_grid": draw_image_grid(jax.random.fold_in(seeds[11], 71), 0),
        "image_owner": draw_image_owner(jax.random.fold_in(seeds[11], 71), 0),
        "row_start": draw_row_start(jax.random.fold_in(seeds[11], 71), 0),
        "merger_pre": gaussian(seeds[4], (MROWS, N_SEQ, HID), 1.0, 6.0, ((1, 16), (2, 2))),
        "vit_out": gaussian(seeds[5], (PSLOT, N_SEQ, VIT), 1.0, 6.0, ((1, 16),)),
        "vit_pre": gaussian(seeds[6], (PSLOT, N_SEQ, VHID), 1.0, 6.0, ((1, 16), (2, 2))),
        "ln_gain": jnp.clip(1.0 + 0.15 * jax.random.normal(seeds[7], (VIT,), jnp.float32), 0.25, 1.75),
        "merger_out_w": gaussian(seeds[8], (D_LLM, HID), D_LLM ** -0.5, 0.0625, ((0, 16), (1, 2))),
        "merger_in_w": gaussian(seeds[9], (HID, MERGE_IN), HID ** -0.5, 0.125, ((0, 2), (1, 16))),
        "vit_fc2_w": gaussian(seeds[10], (VIT, VHID), VIT ** -0.5, 0.15625, ((0, 16), (1, 2))),
    }


def gelu_slope(values):
    return 0.5 * (1.0 + lax.erf(values * 0.7071067811865476)) + values * jnp.exp(-0.5 * values * values) * 0.3989422804014327

def patch_table(widths, counts, slots):
    places = jnp.arange(4 * slots, dtype=jnp.int32)
    merged = places // 4
    corner = places % 4
    row_in = merged[None, :] // widths[:, None]
    col_in = merged[None, :] % widths[:, None]
    target = (2 * row_in + corner[None, :] // 2) * (2 * widths[:, None]) + 2 * col_in + corner[None, :] % 2
    usable = merged[None, :] < counts[:, None]
    return ((target[:, None, :] == places[None, :, None]) & usable[:, None, :]).astype(jnp.float32)

def norm_backward(upstream, inputs, scales):
    average = lax.optimization_barrier(jnp.mean(inputs, -1, keepdims=True))
    centred = inputs - average
    inverse_std = lax.rsqrt(lax.optimization_barrier(jnp.mean(centred * centred, -1, keepdims=True)) + 1e-06)
    normed = centred * inverse_std
    scaled = upstream * scales
    return inverse_std * (scaled - lax.optimization_barrier(jnp.mean(scaled, -1, keepdims=True)) - normed * lax.optimization_barrier(jnp.mean(scaled * normed, -1, keepdims=True)))

def reference(llm_grad, image_grid, image_owner, row_start, merger_pre, vit_out, vit_pre, ln_gain, merger_out_w, merger_in_w, vit_fc2_w):
    grids = image_grid.reshape(N_SEQ, N_SEQ, 2)
    counts = grids[:, :, 0] * grids[:, :, 1]
    widths = grids[:, :, 1]
    owners = image_owner.reshape(N_SEQ, N_SEQ)
    starts = row_start.reshape(N_SEQ, N_SEQ)
    block_width = HID // N_GRP
    sources = jnp.arange(N_SEQ, dtype=jnp.int32)
    within = jnp.arange(SLOT, dtype=jnp.int32)
    in_blocks = merger_in_w.reshape(N_GRP, block_width, MERGE_IN).astype(jnp.float32)

    def one_owner(weight_grad, owner_id):
        chosen = (owners == owner_id).astype(jnp.int32)
        own_counts = lax.optimization_barrier(jnp.sum(chosen * counts, 1))
        own_widths = lax.optimization_barrier(jnp.sum(chosen * widths, 1))
        own_starts = lax.optimization_barrier(jnp.sum(chosen * starts, 1))
        indices = sources[:, None] * SEQ_TOK + jnp.minimum(own_starts[:, None] + within[None, :], SEQ_TOK - 1)
        usable = within[None, :] < own_counts[:, None]
        picked = jnp.take(llm_grad, indices.reshape(-1).astype(jnp.int32), axis=0)
        returned = jnp.where(usable.reshape(-1, 1), picked, jnp.zeros_like(picked))
        hidden_grad = jnp.dot(returned, merger_out_w, preferred_element_type=jnp.float32).astype(jnp.bfloat16)
        pre_act = merger_pre[:, owner_id, :].astype(jnp.float32)
        pre_grad = (gelu_slope(pre_act) * hidden_grad.astype(jnp.float32)).astype(jnp.bfloat16)
        partial_sums = jnp.einsum('rgh,ghc->grc', pre_grad.astype(jnp.float32).reshape(MROWS, N_GRP, block_width), in_blocks)
        rounded = lax.optimization_barrier(partial_sums.astype(jnp.bfloat16))
        merged_grad = lax.optimization_barrier(jnp.sum(rounded.astype(jnp.float32), 0))
        table = patch_table(own_widths, own_counts, SLOT)
        patch_in = jnp.einsum('spq,sqc->spc', table, merged_grad.reshape(N_SEQ, 4 * SLOT, VIT), precision=lax.Precision.HIGHEST).reshape(PSLOT, VIT)
        patch_grad = norm_backward(patch_in, vit_out[:, owner_id, :].astype(jnp.float32), ln_gain).astype(jnp.bfloat16)
        fc_in = vit_pre[:, owner_id, :].astype(jnp.float32)
        sigmoid_q = jax.nn.sigmoid(1.702 * fc_in)
        activation = (fc_in * sigmoid_q).astype(jnp.bfloat16)
        act_grad = jnp.dot(patch_grad, vit_fc2_w, preferred_element_type=jnp.float32)
        fc1_grad = ((sigmoid_q + 1.702 * fc_in * sigmoid_q * (1.0 - sigmoid_q)) * act_grad).astype(jnp.bfloat16)
        weight_grad = weight_grad + lax.dot_general(patch_grad, activation, (((0,), (0,)), ((), ())), preferred_element_type=jnp.float32)
        return (weight_grad, (patch_grad, fc1_grad))
    weight_grad, stacked = lax.scan(one_owner, jnp.zeros((VIT, VHID), jnp.float32), sources)
    return (jnp.transpose(stacked[0], (1, 0, 2)), jnp.transpose(stacked[1], (1, 0, 2)), weight_grad)
```

```python
import jax
import jax.numpy as jnp
from jax import lax
from jax.sharding import PartitionSpec as P

SLOT = 3


def gelu_slope(values):
    return (
        0.5 * (1.0 + lax.erf(values * 0.7071067811865476))
        + values * jnp.exp(-0.5 * values * values) * 0.3989422804014327
    )


def patch_table(widths, counts, slots):
    places = jnp.arange(4 * slots, dtype=jnp.int32)
    merged = places // 4
    corner = places % 4
    row_in = merged[None, :] // widths[:, None]
    col_in = merged[None, :] % widths[:, None]
    target = (
        (2 * row_in + corner[None, :] // 2) * (2 * widths[:, None])
        + 2 * col_in
        + corner[None, :] % 2
    )
    usable = merged[None, :] < counts[:, None]
    return ((target[:, None, :] == places[None, :, None]) & usable[:, None, :]).astype(jnp.float32)


def norm_backward(upstream, inputs, scales):
    average = jnp.mean(inputs, -1, keepdims=True)
    centred = inputs - average
    inverse_std = lax.rsqrt(jnp.mean(centred * centred, -1, keepdims=True) + 1e-06)
    normed = centred * inverse_std
    scaled = upstream * scales
    return inverse_std * (
        scaled
        - jnp.mean(scaled, -1, keepdims=True)
        - normed * jnp.mean(scaled * normed, -1, keepdims=True)
    )


def on_device(
    llm_grad,
    image_grid,
    image_owner,
    row_start,
    merger_pre,
    vit_out,
    vit_pre,
    ln_gain,
    merger_out_w,
    merger_in_w,
    vit_fc2_w,
):
    seq_count = lax.axis_size("seq")
    own_index = lax.axis_index("seq")
    grids = image_grid.reshape(seq_count, seq_count, 2)
    counts = grids[:, :, 0] * grids[:, :, 1]
    widths = grids[:, :, 1]
    owners = image_owner.reshape(seq_count, seq_count)
    starts = row_start.reshape(seq_count, seq_count)
    within = jnp.arange(SLOT, dtype=jnp.int32)
    peers = jnp.arange(seq_count, dtype=jnp.int32)
    shard_rows = llm_grad.shape[0]
    my_owners = lax.dynamic_index_in_dim(owners, own_index, 0, keepdims=False)
    my_counts = lax.dynamic_index_in_dim(counts, own_index, 0, keepdims=False)
    my_starts = lax.dynamic_index_in_dim(starts, own_index, 0, keepdims=False)
    targets = (my_owners[None, :] == peers[:, None]).astype(jnp.int32)
    send_counts = jnp.sum(targets * my_counts[None, :], 1)
    send_starts = jnp.sum(targets * my_starts[None, :], 1)
    indices = jnp.minimum(send_starts[:, None] + within[None, :], shard_rows - 1)
    usable = within[None, :] < send_counts[:, None]
    picked = jnp.take(llm_grad, indices.reshape(-1), axis=0)
    outgoing = jnp.where(usable.reshape(-1, 1), picked, jnp.zeros_like(picked)).reshape(
        seq_count, SLOT, llm_grad.shape[1]
    )
    received = (owners == own_index).astype(jnp.int32)
    recv_counts = jnp.sum(received * counts, 1)
    recv_widths = jnp.sum(received * widths, 1)
    wide_rows = lax.all_gather(
        outgoing.reshape(-1, llm_grad.shape[1]), "grp", axis=1, tiled=True
    )
    sliced = lax.all_to_all(wide_rows, "seq", split_axis=1, concat_axis=0, tiled=True)
    features = sliced.shape[1]
    by_owner = jnp.swapaxes(
        sliced.reshape(seq_count, seq_count, SLOT, features), 0, 1
    ).reshape(-1, features)
    folded = jnp.dot(by_owner, merger_out_w, preferred_element_type=jnp.float32)
    arrived = lax.all_to_all(
        folded.astype(jnp.bfloat16), "seq", split_axis=0, concat_axis=0, tiled=True
    )
    unit_grad = jnp.sum(
        arrived.reshape(seq_count, seq_count * SLOT, -1).astype(jnp.float32), 0
    ).astype(jnp.bfloat16)
    pre_act = merger_pre[:, 0, :].astype(jnp.float32)
    pre_grad = (gelu_slope(pre_act) * unit_grad.astype(jnp.float32)).astype(jnp.bfloat16)
    all_pre = lax.all_gather(pre_grad, "seq", axis=0, tiled=True)
    part_cols = jnp.dot(all_pre, merger_in_w, preferred_element_type=jnp.float32)
    part_rows = lax.all_to_all(
        part_cols.astype(jnp.bfloat16), "seq", split_axis=0, concat_axis=1, tiled=True
    )
    merged_part = jnp.sum(
        lax.all_gather(part_rows, "grp", axis=0).astype(jnp.float32), 0
    )
    vit_width = vit_out.shape[2]
    table = patch_table(recv_widths, recv_counts, SLOT)
    patch_in = jnp.einsum(
        "spq,sqc->spc",
        table,
        merged_part.reshape(seq_count, 4 * SLOT, vit_width),
        precision=lax.Precision.HIGHEST,
    ).reshape(-1, vit_width)
    patch_grad = norm_backward(patch_in, vit_out[:, 0, :].astype(jnp.float32), ln_gain).astype(
        jnp.bfloat16
    )
    group_rows = patch_grad.shape[0] // lax.axis_size("grp")
    own_rows = lax.dynamic_slice_in_dim(
        patch_grad, lax.axis_index("grp") * group_rows, group_rows, 0
    )
    columns = patch_grad
    act_grad = jnp.dot(
        columns,
        lax.all_gather(vit_fc2_w, "seq", axis=0, tiled=True),
        preferred_element_type=jnp.float32,
    )
    fc_in = vit_pre[:, 0, :].astype(jnp.float32)
    sigmoid_q = jax.nn.sigmoid(1.702 * fc_in)
    activation = (fc_in * sigmoid_q).astype(jnp.bfloat16)
    fc1_grad = ((sigmoid_q + 1.702 * fc_in * sigmoid_q * (1.0 - sigmoid_q)) * act_grad).astype(
        jnp.bfloat16
    )
    columns = patch_grad
    weight_part = lax.dot_general(
        columns, activation, (((0,), (0,)), ((), ())), preferred_element_type=jnp.float32
    )
    weight_parts = lax.all_to_all(
        weight_part.astype(jnp.bfloat16), "seq", split_axis=0, concat_axis=0, tiled=True
    )
    weight_grad = jnp.sum(
        weight_parts.reshape(seq_count, -1, weight_part.shape[1]).astype(jnp.float32), 0
    )
    return (
        own_rows.reshape(group_rows, 1, vit_width),
        fc1_grad.reshape(-1, 1, vit_pre.shape[2]),
        weight_grad,
    )


def solution(mesh):
    return jax.shard_map(
        on_device,
        mesh=mesh,
        in_specs=(
            P("seq", "grp"),
            P(),
            P(),
            P(),
            P(None, "seq", "grp"),
            P(None, "seq", None),
            P(None, "seq", "grp"),
            P(),
            P("seq", "grp"),
            P("grp", "seq"),
            P("seq", "grp"),
        ),
        out_specs=(P("grp", "seq", None), P(None, "seq", "grp"), P("seq", "grp")),
        check_vma=False,
    )
```
